256 devices in a mesh: depth: 2 (over y_lo), vx: 16 (over x, y_hi, core), vy: 8 (over z).
Axes of the slice: x: 4, y: 4 (y_hi: 2, y_lo: 2; y = y_hi * 2 + y_lo), z: 8, core: 2. Of those that a mesh axis runs over, the one named last changes fastest.
Arguments:
- token_ids: int32 [1026], replicated, may hold values from 0 to 65535
- hidden: bfloat16 [2, 1024, 7168], P('depth', ('vx', 'vy')), may hold values from -50 to 50
- gain: float32 [2, 7168], P('depth'), may hold values from 0.5 to 1.5
- embedding: bfloat16 [65536, 7168], P('vx', 'vy'), may hold values from -0.6 to 0.6
Outputs:
- row_loss: float32 [1024], P(('vx', 'vy'))
The draws below stay inside these ranges and needn't reach their ends.
All inputs are finite; a program needn't handle non-finite values.
Results may differ from the reference program's by a relative error of at most 0.00044.
Values may be sent and summed in bfloat16 or wider, within the bound.
No kernel may reach another device: no remote copies, remote signals or barrier semaphores. Data moves between devices by JAX's collectives and lax.ppermute only.
A program may use at most 128 MiB of HBM per device.

```python
import math
import jax
import jax.numpy as jnp
from jax import lax

D = 7168
HEADS = 2
VOCAB = 65536
ROWS = 1024


def drawn(key):
    signs = 2.0 * jax.random.randint(jax.random.fold_in(key, 21), (4, D), 0, 2).astype(jnp.float32) - 1.0
    chosen = jax.random.permutation(jax.random.fold_in(key, 22), VOCAB)[:8]
    gaps = jax.random.randint(jax.random.fold_in(key, 23), (4,), 1, 4).astype(jnp.float32)
    return (signs, chosen, gaps)


def draw_embedding(key, part):
    values = jax.random.normal(jax.random.fold_in(key, 11), (VOCAB, D), jnp.float32)
    table = 0.05 * jnp.clip(values, -6.0, 6.0)
    signs, chosen, gaps = drawn(key)
    levels = jnp.array([100.0, 110.0, 120.0, 130.0], jnp.float32)
    upper = signs * (levels / D)[:, None]
    lower = signs * ((levels - gaps) / D)[:, None]
    rows = jnp.stack([upper, lower], axis=1).reshape(8, D)
    table = table.at[chosen].set(rows)
    return table.astype(jnp.bfloat16)


def draw_hidden(key, part):
    base = jnp.clip(jax.random.normal(jax.random.fold_in(key, 12), (HEADS, ROWS, D), jnp.float32), -6.0, 6.0)
    signs, chosen, gaps = drawn(key)
    factors = jax.random.uniform(jax.random.fold_in(key, 24), (HEADS, 4, 1), jnp.float32, 1.0, 20.0)
    aligned = factors * signs[None, :, :]
    picks = jnp.stack([jax.random.permutation(jax.random.fold_in(key, 30 + head), ROWS)[:4] for head in range(HEADS)])
    heads_index = jnp.arange(HEADS)[:, None]
    base = base.at[heads_index, picks].set(aligned)
    return base.astype(jnp.bfloat16)


def touch_ends(entries, key, smallest, top_value):
    extent = entries.shape
    index_at = [jax.random.randint(jax.random.fold_in(key, axis), (), 0, extent[axis]) for axis in range(len(extent))]
    entries = entries.at[tuple(index_at)].set(smallest)
    longest = extent.index(max(extent))
    index_at[longest] = (index_at[longest] + 1) % extent[longest]
    return entries.at[tuple(index_at)].set(top_value)


def setup_inputs(seed: int = 0) -> dict:
    arg_keys = jax.random.split(jax.random.key(seed), 5)
    return {
        "token_ids": touch_ends(jax.random.randint(arg_keys[0], (ROWS + HEADS,), 0, VOCAB), jax.random.fold_in(arg_keys[0], 1), 0, VOCAB - 1).astype(jnp.int32),
        "hidden": draw_hidden(jax.random.fold_in(arg_keys[4], 71), 0),
        "gain": jnp.clip(1.0 + 0.1 * jax.random.normal(arg_keys[2], (HEADS, D), jnp.float32), 0.5, 1.5),
        "embedding": draw_embedding(jax.random.fold_in(arg_keys[4], 71), 0),
    }


EPS = 1e-06

def head_loss(rows, gain_row, embedding, targets):
    values = rows.astype(jnp.float32)
    scale = lax.rsqrt(lax.optimization_barrier(jnp.mean(values * values, axis=1, keepdims=True)) + EPS)
    normed = (values * scale * gain_row[None, :]).astype(jnp.bfloat16)
    block = math.gcd(ROWS, 512)

    def one(pair):
        piece, wanted = pair
        logits = lax.dot_general(piece, embedding, (((1,), (1,)), ((), ())), preferred_element_type=jnp.float32)
        peak = lax.optimization_barrier(jnp.max(logits, axis=1))
        total = lax.optimization_barrier(jnp.sum(jnp.exp(logits - peak[:, None]), axis=1))
        picked = jnp.take_along_axis(logits, wanted[:, None], axis=1)[:, 0]
        return peak + jnp.log(total) - picked
    losses = lax.map(one, (normed.reshape(-1, block, D), targets.reshape(-1, block)))
    return losses.reshape(-1)

def reference(token_ids, hidden, gain, embedding):
    summed = jnp.zeros((ROWS,), jnp.float32)
    for head in range(HEADS):
        targets = token_ids[head + 1:head + 1 + ROWS]
        summed = summed + head_loss(hidden[head], gain[head], embedding, targets)
    return summed
```

```python
import functools

import jax
import jax.numpy as jnp
from jax import lax
from jax.experimental import pallas as pl
from jax.experimental.pallas import tpu as pltpu
from jax.sharding import Mesh
from jax.sharding import PartitionSpec as P

VX = ("vx_0", "vx_1", "vx_2")
VX_VY = ("vx_0", "vx_1", "vx_2", "vy")
ALL = ("depth", "vx_0", "vx_1", "vx_2", "vy")
EPS = 1e-06


def shifted(array, axis, by):
    n = lax.axis_size(axis)
    return lax.ppermute(array, axis, [((i + by) % n, i) for i in range(n)])


def loss_kernel(row_blocks, table_parts, *refs):
    count = 1 + 1 + len(row_blocks) + len(table_parts)
    targets_ref, own_ref = refs[:2]
    row_refs = refs[2 : 2 + len(row_blocks)]
    table_refs = refs[2 + len(row_blocks) : count]
    out_ref, normed, table, row_sems, table_sems = refs[count:]
    depth = lax.axis_index("depth")
    x, yh, core = (lax.axis_index(name) for name in VX)
    z = lax.axis_index("vy")
    width = own_ref.shape[1]
    vocab = table.shape[0]
    half = vocab // 2

    def columns(dz):
        return pl.ds(pl.multiple_of(lax.rem(z + dz, 8) * width, width), width)

    copies = []
    own = pltpu.make_async_copy(
        own_ref.at[pl.ds(pl.multiple_of(z * vocab, vocab), vocab)],
        table.at[:, columns(0)],
        table_sems.at[0],
    )
    own.start()
    copies.append(own)
    for k, (ref, (dz, which)) in enumerate(zip(table_refs, table_parts)):
        if which is None:
            rows = pl.ds(0, vocab)
        else:
            part = depth if which == 0 else 1 - depth
            rows = pl.ds(pl.multiple_of(part * half, half), half)
        copy = pltpu.make_async_copy(ref, table.at[rows, columns(dz)], table_sems.at[k + 1])
        copy.start()
        copies.append(copy)
    row_copies = []
    for k, (ref, (dx, dyh, dcore, first)) in enumerate(zip(row_refs, row_blocks)):
        block = (lax.rem(x + dx, 4) * 2 + lax.rem(yh + dyh, 2)) * 2 + lax.rem(core + dcore, 2)
        at = pl.multiple_of(block * 64 + first, 32)
        copy = pltpu.make_async_copy(ref, normed.at[pl.ds(at, ref.shape[0])], row_sems.at[k])
        copy.start()
        row_copies.append(copy)
    for copy in copies:
        copy.wait()
    for copy in row_copies:
        copy.wait()
    piece = 256
    for at in range(0, normed.shape[0], piece):
        logits = lax.dot_general(
            table[...],
            normed[at : at + piece, :],
            (((1,), (1,)), ((), ())),
            preferred_element_type=jnp.float32,
        )
        wanted = targets_ref[0:1, at : at + piece]
        rows = lax.broadcasted_iota(jnp.int32, logits.shape, 0)
        peak = jnp.max(logits, axis=0, keepdims=True)
        total = jnp.sum(jnp.exp(logits - peak), axis=0, keepdims=True)
        picked = jnp.sum(jnp.where(rows == wanted, logits, 0.0), axis=0, keepdims=True)
        out_ref[0:1, at : at + piece] = peak
        out_ref[1:2, at : at + piece] = total
        out_ref[2:3, at : at + piece] = picked


def body(token_ids, hidden, gain, embedding):
    head = lax.axis_index("depth")
    z = lax.axis_index("vy")
    rows_dev, width = hidden.shape[1:]
    groups = lax.axis_size(VX) * lax.axis_size("vy")
    total_rows = rows_dev * groups
    vx_index = lax.axis_index(VX)
    cycle_index = vx_index * lax.axis_size("vy") + z
    vocab = embedding.shape[0] // lax.axis_size("vy")
    half = vocab // 2
    values = hidden[0].astype(jnp.float32)
    scale = lax.rsqrt(jnp.mean(values * values, axis=1, keepdims=True) + EPS)
    normed = (values * scale * gain[0][None, :]).astype(jnp.bfloat16)

    opposite = shifted(normed, "vy", 4)
    both = jnp.concatenate([normed, opposite])
    after = shifted(both, "vy", 1)
    before = shifted(both, "vy", -1)
    after2 = shifted(after[:rows_dev], "vy", 1)
    before2 = shifted(before[:rows_dev], "vy", -1)
    plane = jnp.concatenate(
        [normed, after[:rows_dev], after2, before[rows_dev:], opposite, after[rows_dev:], before2, before[:rows_dev]]
    )
    other = shifted(plane, "vx_1", 1)
    row_parts = []
    for dyh, mine in ((0, plane), (1, other)):
        right = shifted(mine, "vx_0", 1)
        left = shifted(mine, "vx_0", -1)
        far_top = shifted(right[:32], "vx_0", 1)
        far_low = shifted(left[32:], "vx_0", -1)
        row_parts += [
            ((0, dyh, 0), mine),
            ((1, dyh, 0), right),
            ((3, dyh, 0), left),
            ((2, dyh, 0, 0), far_top),
            ((2, dyh, 0, 32), far_low),
        ]
    rows = []
    for where, part in row_parts:
        first = where[3] if len(where) > 3 else 0
        rows.append(((*where[:2], 0, first), part))
        rows.append(((*where[:2], 1, first), shifted(part, "vx_2", 1)))

    parts = []
    for dz in (4, 3, -3, 2, -2):
        to = lax.rem(z - dz + 8, 8)
        sent = lax.dynamic_slice_in_dim(embedding, to * vocab + head * half, half)
        got = lax.ppermute(sent, "vy", [((i + dz) % 8, i) for i in range(8)])
        parts.append(((dz % 8, 0), got))
        parts.append(((dz % 8, 1), shifted(got, "depth", 1)))
    for dz in (1, -1):
        to = lax.rem(z - dz + 8, 8)
        sent = lax.dynamic_slice_in_dim(embedding, to * vocab, vocab)
        parts.append(((dz % 8, None), lax.ppermute(sent, "vy", [((i + dz) % 8, i) for i in range(8)])))

    targets = lax.dynamic_slice_in_dim(token_ids, head + 1, total_rows) - cycle_index * vocab
    targets = targets.reshape(-1, 8, rows_dev)
    targets = lax.dynamic_slice_in_dim(jnp.concatenate([targets, targets], axis=1), z, 8, axis=1)
    targets = jnp.broadcast_to(targets.reshape(1, total_rows), (8, total_rows))
    hbm = pl.BlockSpec(memory_space=pl.ANY)
    vmem = pl.BlockSpec(memory_space=pltpu.VMEM)
    stats = pl.pallas_call(
        functools.partial(loss_kernel, tuple(w for w, _ in rows), tuple(w for w, _ in parts)),
        out_shape=jax.ShapeDtypeStruct((8, total_rows), jnp.float32),
        in_specs=[vmem] + [hbm] * (1 + len(rows) + len(parts)),
        out_specs=vmem,
        scratch_shapes=[
            pltpu.VMEM((total_rows, width), jnp.bfloat16),
            pltpu.VMEM((vocab, width), jnp.bfloat16),
            pltpu.SemaphoreType.DMA((len(rows),)),
            pltpu.SemaphoreType.DMA((len(parts) + 1,)),
        ],
        compiler_params=pltpu.CompilerParams(vmem_limit_bytes=40 * 2**20),
        cost_estimate=pl.CostEstimate(
            flops=2 * total_rows * vocab * width,
            bytes_accessed=2 * (total_rows + vocab) * width,
            transcendentals=total_rows * vocab,
        ),
    )(targets, embedding, *(p for _, p in rows), *(p for _, p in parts))
    stats = stats[:3].reshape(3, -1, 8, rows_dev)
    stats = lax.dynamic_slice_in_dim(jnp.concatenate([stats, stats], axis=2), lax.rem(8 - z, 8), 8, axis=2)
    stats = stats.reshape(3, groups, rows_dev).transpose(1, 0, 2).reshape(groups, 3 * rows_dev)
    stats = lax.all_to_all(jnp.concatenate([stats, stats]), ALL, 0, 0, tiled=True)
    peak, total, picked = stats.reshape(2, groups, 3, rows_dev).transpose(2, 0, 1, 3)
    top = jnp.max(peak, axis=1, keepdims=True)
    total = jnp.sum(total * jnp.exp(peak - top), axis=1)
    loss = top[:, 0] + jnp.log(total) - jnp.sum(picked, axis=1)
    return loss[0] + loss[1]


def solution(mesh):
    split = Mesh(
        mesh.devices.reshape(mesh.shape["depth"], 4, 2, 2, mesh.shape["vy"]),
        ("depth", "vx_0", "vx_1", "vx_2", "vy"),
    )
    in_specs = (P(), P("depth", VX_VY, None), P("depth", None), P(VX, "vy"))
    out_specs = P(VX_VY)
    return jax.shard_map(body, mesh=split, in_specs=in_specs, out_specs=out_specs, check_vma=False)
```
